512 devices in a mesh: expert: 32 (over z, y_hi), tensor: 16 (over y_lo, x, core).
Axes of the slice: x: 4, y: 8 (y_hi: 4, y_lo: 2; y = y_hi * 2 + y_lo), z: 8, core: 2. Of those that a mesh axis runs over, the one named last changes fastest.
Arguments:
- tokens: bfloat16 [4096, 3072], P('expert', 'tensor'), may hold values from -6 to 6
- expert_ids: int32 [4096, 2], P('expert'), may hold values from 0 to 7, all different within a row; in each aligned block of 128 rows (0 to 127, 128 to 255, ...) at most 48 rows name the same one
- joined_weight: bfloat16 [32, 3072, 2, 4096], P('expert', 'tensor'), may hold values from -0.109375 to 0.109375
Outputs:
- hidden: bfloat16 [4096, 2, 4, 4096], P('expert', None, None, 'tensor')
The draws below stay inside these ranges and needn't reach their ends.
Inputs may be any that keep to these rules, and one draw needn't show every extreme that they name: `expert_ids`: each row names 2 different experts. Among the rows of one device (each aligned block of 128 rows) no expert is named by more than 48 rows, and in some blocks one expert is named by exactly 48 rows.
All inputs are finite; a program needn't handle non-finite values.
Results may differ from the reference program's by a relative error of at most 0.001.
Values may be sent and summed in bfloat16 or wider, within the bound.
No kernel may reach another device: no remote copies, remote signals or barrier semaphores. Data moves between devices by JAX's collectives and lax.ppermute only.
A program may use at most 128 MiB of HBM per device.

```python
import math
import jax
import jax.numpy as jnp
import numpy as np
from jax import lax

E = 8
TOP = 2
D = 3072
FF = 16384
TOK_DEV = 128
CAP = 48
REP = 4
FB = 4096
EB = 32
TOKENS = 4096


def levels(own_key, dims, cuts, low, high):
    loudness = 1.0
    for dim, blocks in cuts:
        steps = jax.random.uniform(jax.random.fold_in(jax.random.fold_in(own_key, 6), dim), (blocks,), jnp.float32, low / len(cuts), high / len(cuts))
        loudness = loudness * jnp.repeat(jnp.exp(steps), dims[dim] // blocks).reshape((-1,) + (1,) * (len(dims) - 1 - dim))
    return loudness


def shared_out(key, own, number, rows, amount, top, bound, lean):
    order = jax.random.permutation(key, amount)
    crowded, usual = load_shares(amount, rows * top, bound, lean, True), load_shares(amount, rows * top, bound, lean, False)
    places = jnp.arange(amount)

    def named(tallies, rotation):
        used = int((tallies > 0).sum())
        fixed = max(1, used // 4)
        passed = fixed + (places - fixed + rotation * (used - fixed)) % max(1, amount - fixed)
        return jnp.zeros((amount,), jnp.int32).at[order[jnp.where(places < fixed, places, passed)]].set(jnp.asarray(tallies, jnp.int32))

    tallies = jnp.where(number % 4 == 0, named(crowded, number // 4), named(usual, number - number // 4 - 1))
    mixed = jax.random.permutation(jax.random.fold_in(own, 3), amount)
    giver, sink = mixed[0:amount // 2 * 2:2], mixed[1:amount // 2 * 2:2]
    margin = jnp.minimum(tallies[giver] - 1, bound - tallies[sink]) // 2
    margin = jnp.where((giver == order[0]) | (sink == order[0]) | (tallies[sink] == 0), 0, jnp.maximum(margin, 0))
    passed = jax.random.randint(jax.random.fold_in(own, 4), (amount // 2,), 0, 1 << 20) % (margin + 1)
    tallies = tallies.at[giver].add(-passed).at[sink].add(passed)
    labels = jnp.searchsorted(jnp.cumsum(tallies), jnp.arange(rows * top), side="right").astype(jnp.int32)
    listing = labels.reshape(top, rows).T
    listing = listing[jax.random.permutation(jax.random.fold_in(own, 1), rows)]
    rotation = jax.random.randint(jax.random.fold_in(own, 2), (rows, 1), 0, top)
    return jnp.take_along_axis(listing, (jnp.arange(top)[None, :] + rotation) % top, axis=1)


def load_shares(amount, total, bound, lean, full):
    portions = [(1 << 20) // math.isqrt(standing ** lean) + 1 for standing in range(1, amount + 1)]
    largest = bound if full else min(bound, max(-(-total // amount), total * portions[0] // sum(portions)))
    least = 1 if total - largest >= amount - 1 else 0
    holding, spare = [largest] + [least] * (amount - 1), total - largest - least * (amount - 1)
    while spare > 0:
        free = [i for i in range(1, amount) if holding[i] < largest] or [i for i in range(1, amount) if holding[i] < bound]
        mass, remaining = sum([portions[i] for i in free]), spare
        for i in free:
            addition = min(bound - holding[i], max(1, remaining * portions[i] // mass), spare)
            holding[i] = holding[i] + addition
            spare = spare - addition
    return np.array(holding)


def gaussian(rng, shape, deviation, reach, split=(), kind=jnp.bfloat16):
    drawn = jax.random.normal(rng, shape, jnp.float32) * deviation
    if len(split) > 0:
        drawn = levels(rng, shape, split, -0.22, 0.18) * drawn
    return jnp.clip(drawn, min=-reach, max=reach).astype(kind)


def setup_inputs(seed: int = 0) -> dict:
    key_of = jax.random.split(jax.random.key(seed), 4)
    tokens = gaussian(key_of[0], (TOKENS, D), 1.0, 6.0, ((0, 32), (1, 16)))
    expert_ids_keys = jax.random.split(jax.random.fold_in(key_of[1], 1), TOKENS // TOK_DEV)
    expert_ids_turns = jax.random.permutation(jax.random.fold_in(key_of[1], 3), TOKENS // TOK_DEV)
    expert_ids = jax.vmap(lambda own, number: shared_out(jax.random.fold_in(key_of[1], 2), own, number, TOK_DEV, E, TOP, CAP, 2))(expert_ids_keys, expert_ids_turns).reshape((TOKENS, TOP))
    joined_weight = gaussian(key_of[2], (EB, D, 2, FB), D ** -0.5, 0.109375, ((0, 32), (1, 16)))
    return {"tokens": tokens, "expert_ids": expert_ids, "joined_weight": joined_weight}


def reference(tokens, expert_ids, joined_weight):
    sources = TOKENS // TOK_DEV
    flat_ids = expert_ids.reshape(sources, TOK_DEV * TOP)
    chosen = (flat_ids[:, :, None] == jnp.arange(E, dtype=jnp.int32)[None, None, :]).astype(jnp.int32)
    earlier = jnp.cumsum(chosen, axis=1) - chosen
    position = jnp.sum(earlier * chosen, axis=2).astype(jnp.int32)
    slot_index = (jnp.arange(sources, dtype=jnp.int32)[:, None] * CAP + position).reshape(-1).astype(jnp.int32)
    all_ids = flat_ids.reshape(-1)
    token_of = (jnp.arange(TOKENS * TOP, dtype=jnp.int32) // TOP).astype(jnp.int32)
    routed = tokens[token_of]

    def one_expert(index, result):
        expert = jnp.asarray(index).astype(jnp.int32)
        w_block = lax.dynamic_slice_in_dim(joined_weight, (expert * REP).astype(jnp.int32), REP, 0)
        weight = jnp.transpose(w_block, (1, 2, 0, 3)).reshape(D, 2 * FF)
        is_mine = all_ids == expert
        target = jnp.where(is_mine, slot_index, sources * CAP).astype(jnp.int32)
        buffer = jnp.zeros((sources * CAP + 1, D), jnp.bfloat16).at[target].set(routed)
        gate_up = jnp.dot(buffer, weight, preferred_element_type=jnp.float32)
        active = (jax.nn.silu(gate_up[:, :FF]) * gate_up[:, FF:]).astype(jnp.bfloat16)
        return jnp.where(is_mine[:, None], active[target], result)

    start_out = jnp.zeros((TOKENS * TOP, FF), jnp.bfloat16)
    result = lax.fori_loop(0, E, one_expert, start_out)
    return result.reshape(TOKENS, TOP, REP, FB)
```

```python
import jax
import jax.numpy as jnp
from jax import lax
from jax.experimental import pallas as pl
from jax.experimental.pallas import tpu as pltpu
from jax.sharding import Mesh, PartitionSpec as P

E = 8
TOP = 2
CAP = 48
GROUPS = ((0,), (1, 3), (2,))


EXPERT = ("z", "yh")
TENSOR = ("yl", "x", "c")
SWAP = [(0, 1), (1, 0)]


def shift(axis, by):
    n = lax.axis_size(axis)
    return [(i, (i + by) % n) for i in range(n)]


def split_kernel(w_ref, out_ref, sems):
    chips, width = out_ref.shape[0], out_ref.shape[3]
    copies = [
        pltpu.make_async_copy(
            w_ref.at[0, :, :, pl.ds(p * width, width)], out_ref.at[p], sems.at[p]
        )
        for p in range(chips)
    ]
    for copy in copies:
        copy.start()
    for copy in copies:
        copy.wait()


def split_columns(joined_weight, chips):
    _, rows, two, columns = joined_weight.shape
    shape = (chips, rows, two, columns // chips)
    return pl.pallas_call(
        split_kernel,
        out_shape=jax.ShapeDtypeStruct(shape, joined_weight.dtype),
        in_specs=[pl.BlockSpec(memory_space=pl.ANY)],
        out_specs=pl.BlockSpec(memory_space=pltpu.VMEM),
        scratch_shapes=[pltpu.SemaphoreType.DMA((chips,))],
        cost_estimate=pl.CostEstimate(flops=10**9, bytes_accessed=2 * 3 * 2**20, transcendentals=0),
        compiler_params=pltpu.CompilerParams(vmem_limit_bytes=8 * 2**20),
    )(joined_weight)


def hidden_kernel(groups, place, w_own, w_other, *refs):
    pieces, out = refs[: 5 * len(groups)], refs[-1]
    zs, cores, xs = 8, 2, 4
    n, half_width = out.shape[1], out.shape[2]
    height = zs * n
    depth = w_own.shape[0] // (2 * xs)
    for g, members in enumerate(groups):
        own, low, high, far_a, far_b = pieces[5 * g : 5 * g + 5]
        cut = far_a.shape[0]
        for i, m in enumerate(members):
            start, stop = i * height, (i + 1) * height
            rows = slice(start, stop)
            if stop <= cut:
                far = far_a[rows]
            elif start >= cut:
                far = far_b[start - cut : stop - cut]
            else:
                far = jnp.concatenate([far_a[start:cut], far_b[: stop - cut]], axis=0)
            for w, c in ((w_own, place[4]), (w_other, place[5])):
                total = jnp.zeros((height, 2 * half_width), jnp.float32)
                for k, x in enumerate((own[rows], low[rows], high[rows], far)):
                    for side in range(2):
                        at = pl.multiple_of((side * xs + place[k]) * depth, depth)
                        total = total + jnp.dot(
                            x[:, side * depth : (side + 1) * depth],
                            w[pl.ds(at, depth)],
                            preferred_element_type=jnp.float32,
                        )
                gate, up = total[:, :half_width], total[:, half_width:]
                active = (gate / (1.0 + jnp.exp(-gate)) * up).astype(jnp.bfloat16)
                for z in range(zs):
                    out[place[6 + m] * (zs * cores) + place[10 + z] * cores + c] = active[
                        z * n : (z + 1) * n
                    ]


def hidden_blocks(place, pieces, w_own, w_other, groups, n, half_width, held=None):
    vmem = pl.BlockSpec(memory_space=pltpu.VMEM)
    pieces = [p for group in pieces for p in group]
    inputs = [place, w_own, w_other] + pieces + ([] if held is None else [held])
    rows = 192 * sum(len(members) for members in groups)
    return pl.pallas_call(
        lambda *refs: hidden_kernel(groups, *refs),
        out_shape=jax.ShapeDtypeStruct((64, n, half_width), jnp.bfloat16),
        in_specs=[pl.BlockSpec(memory_space=pltpu.SMEM)] + [vmem] * (len(inputs) - 1),
        out_specs=vmem,
        input_output_aliases={} if held is None else {len(inputs) - 1: 0},
        cost_estimate=pl.CostEstimate(
            flops=2 * rows * 3072 * 1024, bytes_accessed=2 * rows * 3072, transcendentals=rows * 512
        ),
        compiler_params=pltpu.CompilerParams(vmem_limit_bytes=12 * 2**20),
    )(*inputs)


def gather_x(block):
    half = block.shape[0] // 2
    low = lax.ppermute(block, "x", shift("x", 1))
    high = lax.ppermute(block, "x", shift("x", -1))
    low_part, high_part = low[:half], high[half:]
    far_a = lax.ppermute(low_part, "x", shift("x", 1))
    far_b = lax.ppermute(high_part, "x", shift("x", -1))
    return block, low, high, far_a, far_b


def local(tokens, expert_ids, joined_weight):
    zs, copies = lax.axis_size("z"), lax.axis_size("yh")
    yls, xs, cores = lax.axis_size("yl"), lax.axis_size("x"), lax.axis_size("c")
    chips = yls * xs
    part = CAP // cores
    core = lax.axis_index("c")
    here = lax.axis_index("x")
    row = lax.axis_index("yh")
    side = lax.axis_index("yl")
    depth = lax.axis_index("z")
    rows = joined_weight.shape[1]
    chip_width = joined_weight.shape[3] // chips
    half_width = chip_width // cores

    tok_count = tokens.shape[0]
    flat_ids = expert_ids.reshape(-1)
    chosen = (flat_ids[:, None] == jnp.arange(E, dtype=jnp.int32)[None, :]).astype(jnp.int32)
    earlier = jnp.cumsum(chosen, axis=0) - chosen
    position = jnp.sum(earlier * chosen, axis=1)
    slot_index = flat_ids * CAP + position
    slots = jnp.arange(E * CAP, dtype=jnp.int32)
    pick_table = (slot_index[:, None] == slots[None, :]).astype(jnp.bfloat16)

    tok_c = lax.ppermute(tokens, "c", SWAP)
    tok_y = lax.ppermute(tokens, "yl", SWAP)
    tok_yc = lax.ppermute(tokens, ("yl", "c"), [(i, 3 - i) for i in range(4)])
    near = [jnp.where(core == 0, tokens, tok_c), jnp.where(core == 0, tok_c, tokens)]
    far = [jnp.where(core == 0, tok_y, tok_yc), jnp.where(core == 0, tok_yc, tok_y)]
    wide = [jnp.where(side == 0, p, q) for p, q in zip(near + far, far + near)]
    wide = jnp.concatenate(wide, axis=1)

    turn = jnp.arange(zs, dtype=jnp.int32)
    wanted = lax.rem(depth + turn, zs)[:, None] * CAP + core * part
    wanted = (wanted + jnp.arange(part, dtype=jnp.int32)[None, :]).reshape(-1)
    pairs = slot_index.reshape(tok_count, TOP)
    table = (pairs[:, :, None] == wanted[None, None, :]).any(axis=1).astype(jnp.bfloat16)
    placed = lax.dot_general(
        table, wide, (((0,), (0,)), ((), ())), preferred_element_type=jnp.float32
    ).astype(jnp.bfloat16)
    placed = placed.reshape(zs, part, wide.shape[1])
    moved = [placed[0]] + [
        lax.ppermute(placed[s], "z", shift("z", s)) for s in range(1, zs)
    ]
    own = jnp.concatenate(moved, axis=0)
    sources = [own] + [lax.ppermute(own, "yh", shift("yh", s)) for s in range(1, copies)]

    pieces = split_columns(joined_weight, chips * cores)
    w_own = lax.all_to_all(pieces, TENSOR, 0, 0, tiled=True)
    w_own = w_own.reshape(chips * cores * rows, 2 * half_width)
    w_other = lax.ppermute(w_own, "c", SWAP)
    place = jnp.concatenate(
        [
            lax.rem(here + xs + jnp.array([0, -1, 1, 2], jnp.int32), xs),
            jnp.stack([core, 1 - core]),
            lax.rem(row + copies - jnp.arange(copies, dtype=jnp.int32), copies),
            lax.rem(depth + zs - turn, zs),
        ]
    )
    gathered = []
    for members in GROUPS:
        block = jnp.concatenate([sources[m] for m in members], axis=0)
        gathered.append(gather_x(block))
    outgoing = hidden_blocks(
        place, gathered[:2], w_own, w_other, GROUPS[:2], part, half_width
    )
    outgoing = hidden_blocks(
        place, gathered[2:], w_own, w_other, GROUPS[2:], part, half_width, outgoing
    )
    pick_table, outgoing = lax.optimization_barrier((pick_table, outgoing))
    returned = lax.all_to_all(outgoing, ("yh", "z", "c"), 0, 0, tiled=True)
    grouped = returned.reshape(copies, E * CAP, half_width).transpose(1, 0, 2)
    grouped = grouped.reshape(E * CAP, copies * half_width)
    hidden = jnp.dot(pick_table, grouped, preferred_element_type=jnp.float32).astype(jnp.bfloat16)
    return hidden.reshape(tok_count, TOP, copies, half_width)


def solution(mesh):
    fine = Mesh(mesh.devices.reshape(8, 4, 2, 4, 2), ("z", "yh", "yl", "x", "c"))

    return jax.shard_map(
        local,
        mesh=fine,
        in_specs=(P(EXPERT, TENSOR), P(EXPERT, None), P(EXPERT, TENSOR, None, None)),
        out_specs=P(EXPERT, None, None, TENSOR),
        check_vma=False,
    )
```

```python
import jax
import jax.numpy as jnp
from jax import lax
from jax.experimental import pallas as pl
from jax.experimental.pallas import tpu as pltpu
from jax.sharding import Mesh, PartitionSpec as P

E = 8
TOP = 2
CAP = 48


EXPERT = ("z", "yh")
TENSOR = ("yl", "x", "c")
CHIPS = ("yl", "x")
SWAP = [(0, 1), (1, 0)]


def shift(axis, by):
    n = lax.axis_size(axis)
    return [(i, (i + by) % n) for i in range(n)]


def chip_shift(side, by):
    return [(i, (i // 4 + side) % 2 * 4 + (i % 4 + by) % 4) for i in range(8)]


def split_kernel(chip, w_ref, *refs):
    *outs, sems = refs
    width = outs[0].shape[2]
    copies = []
    for p, out in enumerate(outs):
        at = pl.multiple_of(chip[p] * width, width)
        copies.append(pltpu.make_async_copy(w_ref.at[0, :, :, pl.ds(at, width)], out, sems.at[p]))
    for copy in copies:
        copy.start()
    for copy in copies:
        copy.wait()


def split_columns(joined_weight, chip):
    _, rows, two, columns = joined_weight.shape
    chips = chip.shape[0]
    piece = jax.ShapeDtypeStruct((rows, two, columns // chips), joined_weight.dtype)
    vmem = pl.BlockSpec(memory_space=pltpu.VMEM)
    return pl.pallas_call(
        split_kernel,
        out_shape=[piece] * chips,
        in_specs=[pl.BlockSpec(memory_space=pltpu.SMEM), pl.BlockSpec(memory_space=pltpu.HBM)],
        out_specs=[vmem] * chips,
        scratch_shapes=[pltpu.SemaphoreType.DMA((chips,))],
        cost_estimate=pl.CostEstimate(flops=10**9, bytes_accessed=2 * 3 * 2**20, transcendentals=0),
        compiler_params=pltpu.CompilerParams(vmem_limit_bytes=8 * 2**20),
    )(chip, joined_weight)


BLOCK = 192


def add_product(total, x, s, w_mine, w_other, columns):
    w = jnp.concatenate([w_mine[s, :, columns], w_other[s, :, columns]], axis=0)
    return total + jnp.dot(x, w, preferred_element_type=jnp.float32)


def near_kernel(w_mine, w_other, *refs):
    *pieces, out = refs
    width = out.shape[1] // 2
    for start in range(0, out.shape[0], BLOCK):
        rows = slice(start, start + BLOCK)
        for side in range(2):
            columns = slice(side * width, (side + 1) * width)
            total = jnp.zeros((BLOCK, width), jnp.float32)
            for x, s in zip(pieces, (0, 1, 3, 4, 5, 7)):
                total = add_product(total, x[rows], s, w_mine, w_other, columns)
            out[rows, columns] = total


def hidden_kernel(w_mine, w_other, low0, high0, low1, high1, sums, out):
    copies, zs, cores = 4, 8, 2
    n, half_width = out.shape[1], out.shape[2]
    width, cut = cores * half_width, low0.shape[0]
    for start in range(0, sums.shape[0], BLOCK):
        rows = slice(start, start + BLOCK)
        if start < cut:
            x0, x1 = low0[rows], low1[rows]
        else:
            x0, x1 = high0[start - cut : start - cut + BLOCK], high1[start - cut : start - cut + BLOCK]
        for c in range(cores):
            both = []
            for first in (c * half_width, width + c * half_width):
                columns = slice(first, first + half_width)
                total = add_product(sums[rows, columns], x0, 2, w_mine, w_other, columns)
                both.append(add_product(total, x1, 6, w_mine, w_other, columns))
            gate, up = both
            active = (gate / (1.0 + jnp.exp(-gate)) * up).astype(jnp.bfloat16)
            for j in range(BLOCK // n):
                z, row = divmod(start // n + j, copies)
                out[(row * zs + z) * cores + c] = active[j * n : (j + 1) * n]


def on_core(kernel, out_shape, *inputs):
    vmem = pl.BlockSpec(memory_space=pltpu.VMEM)
    return pl.pallas_call(
        kernel,
        out_shape=out_shape,
        in_specs=[vmem] * len(inputs),
        out_specs=vmem,
        cost_estimate=pl.CostEstimate(
            flops=768 * 3072 * 1024, bytes_accessed=6 * 2**20, transcendentals=768 * 512
        ),
        compiler_params=pltpu.CompilerParams(vmem_limit_bytes=12 * 2**20),
    )(*inputs)


def gather_x(block):
    half = block.shape[0] // 2
    low = lax.ppermute(block, "x", shift("x", 1))
    high = lax.ppermute(block, "x", shift("x", -1))
    low_part, high_part = low[:half], high[half:]
    far_a = lax.ppermute(low_part, "x", shift("x", 1))
    far_b = lax.ppermute(high_part, "x", shift("x", -1))
    return block, low, high, far_a, far_b


def local(tokens, expert_ids, joined_weight):
    zs, copies = lax.axis_size("z"), lax.axis_size("yh")
    yls, xs, cores = lax.axis_size("yl"), lax.axis_size("x"), lax.axis_size("c")
    chips = yls * xs
    part = CAP // cores
    core, here, side = lax.axis_index("c"), lax.axis_index("x"), lax.axis_index("yl")
    rows = joined_weight.shape[1]
    chip_width = joined_weight.shape[3] // chips
    half_width = chip_width // cores

    tok_count = tokens.shape[0]
    flat_ids = expert_ids.reshape(-1)
    chosen = (flat_ids[:, None] == jnp.arange(E, dtype=jnp.int32)[None, :]).astype(jnp.int32)
    earlier = jnp.cumsum(chosen, axis=0) - chosen
    position = jnp.sum(earlier * chosen, axis=1)
    slot_index = flat_ids * CAP + position
    slots = jnp.arange(E * CAP, dtype=jnp.int32)
    pick_table = (slot_index[:, None] == slots[None, :]).astype(jnp.bfloat16)
    token_table = pick_table.reshape(tok_count, TOP, E * CAP).sum(axis=1)
    placed = lax.dot_general(
        token_table, tokens, (((0,), (0,)), ((), ())), preferred_element_type=jnp.float32
    ).astype(jnp.bfloat16)

    sent = placed.reshape(zs, 1, cores, part, rows)
    sent = jnp.broadcast_to(sent, (zs, copies, cores, part, rows)).reshape(-1, part, rows)
    got = lax.all_to_all(sent, ("z", "yh", "c"), 0, 0, tiled=True)
    got = got.reshape(zs * copies, cores, part, rows)

    turn = jnp.arange(chips, dtype=jnp.int32)
    chip = lax.rem(side + turn // xs, yls) * xs + lax.rem(here + turn % xs, xs)
    pieces = split_columns(joined_weight, chip)
    moved = [pieces[0]]
    for s in range(1, chips):
        moved.append(lax.ppermute(pieces[s], CHIPS, chip_shift(s // xs, s % xs)))
    mine = jnp.where(core == 0, got[:, 0], got[:, 1])
    theirs = jnp.where(core == 0, got[:, 1], got[:, 0])
    own = jnp.concatenate([mine, theirs], axis=-1).reshape(zs * copies * part, cores * rows)
    opposite = lax.ppermute(own, "yl", SWAP)
    moved, opposite = lax.optimization_barrier((moved, opposite))
    w_mine = jnp.concatenate([m.reshape(rows, 2 * chip_width) for m in moved], axis=0)
    w_other = lax.ppermute(w_mine, "c", SWAP)
    shape = (chips, rows, 2 * chip_width)
    w_mine, w_other = w_mine.reshape(shape), w_other.reshape(shape)

    near = gather_x(own)
    far = gather_x(opposite)
    sums = jax.ShapeDtypeStruct((own.shape[0], 2 * chip_width), jnp.float32)
    half_sums = on_core(near_kernel, sums, w_mine, w_other, *near[:3], *far[:3])
    active = jax.ShapeDtypeStruct((zs * copies * cores, part, half_width), jnp.bfloat16)
    outgoing = on_core(hidden_kernel, active, w_mine, w_other, *near[3:], *far[3:], half_sums)

    pick_table, outgoing = lax.optimization_barrier((pick_table, outgoing))
    returned = lax.all_to_all(outgoing, ("yh", "z", "c"), 0, 0, tiled=True)
    grouped = returned.reshape(copies, E * CAP, half_width).transpose(1, 0, 2)
    grouped = grouped.reshape(E * CAP, copies * half_width)
    hidden = jnp.dot(pick_table, grouped, preferred_element_type=jnp.float32).astype(jnp.bfloat16)
    return hidden.reshape(tok_count, TOP, copies, half_width)


def solution(mesh):
    fine = Mesh(mesh.devices.reshape(8, 4, 2, 4, 2), ("z", "yh", "yl", "x", "c"))

    return jax.shard_map(
        local,
        mesh=fine,
        in_specs=(P(EXPERT, TENSOR), P(EXPERT, None), P(EXPERT, TENSOR, None, None)),
        out_specs=P(EXPERT, None, None, TENSOR),
        check_vma=False,
    )
```

```python
import jax
import jax.numpy as jnp
from jax import lax
from jax.experimental import pallas as pl
from jax.experimental.pallas import tpu as pltpu
from jax.sharding import Mesh, PartitionSpec as P

E = 8
TOP = 2
CAP = 48


EXPERT = ("z", "yh")
TENSOR = ("yl", "x", "c")
CHIPS = ("yl", "x")
SWAP = [(0, 1), (1, 0)]


def shift(axis, by):
    n = lax.axis_size(axis)
    return [(i, (i + by) % n) for i in range(n)]


def chip_shift(side, by):
    return [(i, (i // 4 + side) % 2 * 4 + (i % 4 + by) % 4) for i in range(8)]


def split_kernel(chip, w_ref, *refs):
    *outs, sems = refs
    width = outs[0].shape[2]
    copies = []
    for p, out in enumerate(outs):
        at = pl.multiple_of(chip[p] * width, width)
        copies.append(pltpu.make_async_copy(w_ref.at[0, :, :, pl.ds(at, width)], out, sems.at[p]))
    for copy in copies:
        copy.start()
    for copy in copies:
        copy.wait()


def split_columns(joined_weight, chip):
    _, rows, two, columns = joined_weight.shape
    chips = chip.shape[0]
    piece = jax.ShapeDtypeStruct((rows, two, columns // chips), joined_weight.dtype)
    vmem = pl.BlockSpec(memory_space=pltpu.VMEM)
    return pl.pallas_call(
        split_kernel,
        out_shape=[piece] * chips,
        in_specs=[pl.BlockSpec(memory_space=pltpu.SMEM), pl.BlockSpec(memory_space=pltpu.HBM)],
        out_specs=[vmem] * chips,
        scratch_shapes=[pltpu.SemaphoreType.DMA((chips,))],
        cost_estimate=pl.CostEstimate(flops=10**9, bytes_accessed=2 * 3 * 2**20, transcendentals=0),
        compiler_params=pltpu.CompilerParams(vmem_limit_bytes=8 * 2**20),
    )(chip, joined_weight)


BLOCK = 192


def add_product(total, x, s, w_mine, w_other, columns):
    w = jnp.concatenate([w_mine[s, :, columns], w_other[s, :, columns]], axis=0)
    return total + jnp.dot(x, w, preferred_element_type=jnp.float32)


def near_kernel(w_mine, w_other, *refs):
    *pieces, out = refs
    width = out.shape[1] // 2
    for start in range(0, out.shape[0], BLOCK):
        rows = slice(start, start + BLOCK)
        for side in range(2):
            columns = slice(side * width, (side + 1) * width)
            total = jnp.zeros((BLOCK, width), jnp.float32)
            for x, s in zip(pieces, (0, 1, 3, 4, 5, 7)):
                total = add_product(total, x[rows], s, w_mine, w_other, columns)
            out[rows, columns] = total


def hidden_kernel(w_mine, w_other, low0, high0, low1, high1, sums, out):
    copies, zs, cores = 4, 8, 2
    n, half_width = out.shape[1], out.shape[2]
    width, cut = cores * half_width, low0.shape[0]
    for start in range(0, sums.shape[0], BLOCK):
        rows = slice(start, start + BLOCK)
        if start < cut:
            x0, x1 = low0[rows], low1[rows]
        else:
            x0, x1 = high0[start - cut : start - cut + BLOCK], high1[start - cut : start - cut + BLOCK]
        for c in range(cores):
            both = []
            for first in (c * half_width, width + c * half_width):
                columns = slice(first, first + half_width)
                total = add_product(sums[rows, columns], x0, 2, w_mine, w_other, columns)
                both.append(add_product(total, x1, 6, w_mine, w_other, columns))
            gate, up = both
            active = (gate / (1.0 + jnp.exp(-gate)) * up).astype(jnp.bfloat16)
            for j in range(BLOCK // n):
                z, row = divmod(start // n + j, copies)
                out[(c * zs + z) * copies + row] = active[j * n : (j + 1) * n]


def on_core(kernel, out_shape, *inputs):
    vmem = pl.BlockSpec(memory_space=pltpu.VMEM)
    return pl.pallas_call(
        kernel,
        out_shape=out_shape,
        in_specs=[vmem] * len(inputs),
        out_specs=vmem,
        cost_estimate=pl.CostEstimate(
            flops=768 * 3072 * 1024, bytes_accessed=6 * 2**20, transcendentals=768 * 512
        ),
        compiler_params=pltpu.CompilerParams(vmem_limit_bytes=12 * 2**20),
    )(*inputs)


def gather_x(block):
    half = block.shape[0] // 2
    low = lax.ppermute(block, "x", shift("x", 1))
    high = lax.ppermute(block, "x", shift("x", -1))
    low_part, high_part = low[:half], high[half:]
    far_a = lax.ppermute(low_part, "x", shift("x", 1))
    far_b = lax.ppermute(high_part, "x", shift("x", -1))
    return block, low, high, far_a, far_b


def local(tokens, expert_ids, joined_weight):
    zs, copies = lax.axis_size("z"), lax.axis_size("yh")
    yls, xs, cores = lax.axis_size("yl"), lax.axis_size("x"), lax.axis_size("c")
    chips = yls * xs
    part = CAP // cores
    core, here, side = lax.axis_index("c"), lax.axis_index("x"), lax.axis_index("yl")
    rows = joined_weight.shape[1]
    chip_width = joined_weight.shape[3] // chips
    half_width = chip_width // cores

    tok_count = tokens.shape[0]
    flat_ids = expert_ids.reshape(-1)
    chosen = (flat_ids[:, None] == jnp.arange(E, dtype=jnp.int32)[None, :]).astype(jnp.int32)
    earlier = jnp.cumsum(chosen, axis=0) - chosen
    position = jnp.sum(earlier * chosen, axis=1)
    slot_index = flat_ids * part + position + (position >= part) * (E * part - part)
    slots = jnp.arange(E * CAP, dtype=jnp.int32)
    pick_table = (slot_index[:, None] == slots[None, :]).astype(jnp.bfloat16)
    token_table = pick_table.reshape(tok_count, TOP, E * CAP).sum(axis=1)
    placed = lax.dot_general(
        token_table, tokens, (((0,), (0,)), ((), ())), preferred_element_type=jnp.float32
    ).astype(jnp.bfloat16)

    sent = placed.reshape(cores, zs, 1, part, rows)
    sent = jnp.broadcast_to(sent, (cores, zs, copies, part, rows)).reshape(-1, part, rows)
    got = lax.all_to_all(sent, ("c", "z", "yh"), 0, 0, tiled=True)
    got = got.reshape(cores, zs * copies, part, rows)

    turn = jnp.arange(chips, dtype=jnp.int32)
    chip = lax.rem(side + turn // xs, yls) * xs + lax.rem(here + turn % xs, xs)
    pieces = split_columns(joined_weight, chip)
    moved = [pieces[0]]
    for s in range(1, chips):
        moved.append(lax.ppermute(pieces[s], CHIPS, chip_shift(s // xs, s % xs)))
    mine = jnp.where(core == 0, got[0], got[1])
    theirs = jnp.where(core == 0, got[1], got[0])
    own = jnp.concatenate([mine, theirs], axis=-1).reshape(zs * copies * part, cores * rows)
    opposite = lax.ppermute(own, "yl", SWAP)
    moved, opposite = lax.optimization_barrier((moved, opposite))
    w_mine = jnp.concatenate([m.reshape(rows, 2 * chip_width) for m in moved], axis=0)
    w_other = lax.ppermute(w_mine, "c", SWAP)
    shape = (chips, rows, 2 * chip_width)
    w_mine, w_other = w_mine.reshape(shape), w_other.reshape(shape)

    near = gather_x(own)
    far = gather_x(opposite)
    sums = jax.ShapeDtypeStruct((own.shape[0], 2 * chip_width), jnp.float32)
    half_sums = on_core(near_kernel, sums, w_mine, w_other, *near[:3], *far[:3])
    active = jax.ShapeDtypeStruct((zs * copies * cores, part, half_width), jnp.bfloat16)
    outgoing = on_core(hidden_kernel, active, w_mine, w_other, *near[3:], *far[3:], half_sums)

    pick_table, outgoing = lax.optimization_barrier((pick_table, outgoing))
    returned = lax.all_to_all(outgoing, ("c", "z", "yh"), 0, 0, tiled=True)
    grouped = returned.reshape(cores * E, copies, part, half_width).transpose(0, 2, 1, 3)
    grouped = grouped.reshape(E * CAP, copies * half_width)
    hidden = jnp.dot(pick_table, grouped, preferred_element_type=jnp.float32).astype(jnp.bfloat16)
    return hidden.reshape(tok_count, TOP, copies, half_width)


def solution(mesh):
    fine = Mesh(mesh.devices.reshape(8, 4, 2, 4, 2), ("z", "yh", "yl", "x", "c"))

    return jax.shard_map(
        local,
        mesh=fine,
        in_specs=(P(EXPERT, TENSOR), P(EXPERT, None), P(EXPERT, TENSOR, None, None)),
        out_specs=P(EXPERT, None, None, TENSOR),
        check_vma=False,
    )
```

```python
import jax
import jax.numpy as jnp
from jax import lax
from jax.experimental import pallas as pl
from jax.experimental.pallas import tpu as pltpu
from jax.sharding import Mesh, PartitionSpec as P

E = 8
TOP = 2
CAP = 48


EXPERT = ("z", "yh")
TENSOR = ("yl", "x", "c")
CHIPS = ("yl", "x")
SWAP = [(0, 1), (1, 0)]


def shift(axis, by):
    n = lax.axis_size(axis)
    return [(i, (i + by) % n) for i in range(n)]


def chip_shift(side, by):
    return [(i, (i // 4 + side) % 2 * 4 + (i % 4 + by) % 4) for i in range(8)]


def split_kernel(chip, w_ref, *refs):
    *outs, sems = refs
    width = outs[0].shape[2]
    copies = []
    for p, out in enumerate(outs):
        at = pl.multiple_of(chip[p] * width, width)
        copies.append(pltpu.make_async_copy(w_ref.at[0, :, :, pl.ds(at, width)], out, sems.at[p]))
    for copy in copies:
        copy.start()
    for copy in copies:
        copy.wait()


def split_columns(joined_weight, chip):
    _, rows, two, columns = joined_weight.shape
    chips = chip.shape[0]
    piece = jax.ShapeDtypeStruct((rows, two, columns // chips), joined_weight.dtype)
    vmem = pl.BlockSpec(memory_space=pltpu.VMEM)
    return pl.pallas_call(
        split_kernel,
        out_shape=[piece] * chips,
        in_specs=[pl.BlockSpec(memory_space=pltpu.SMEM), pl.BlockSpec(memory_space=pltpu.HBM)],
        out_specs=[vmem] * chips,
        scratch_shapes=[pltpu.SemaphoreType.DMA((chips,))],
        cost_estimate=pl.CostEstimate(flops=10**9, bytes_accessed=2 * 3 * 2**20, transcendentals=0),
        compiler_params=pltpu.CompilerParams(vmem_limit_bytes=8 * 2**20),
    )(chip, joined_weight)


BLOCK = 192


def add_product(total, x, s, w_mine, w_other, columns):
    w = jnp.concatenate([w_mine[s, :, columns], w_other[s, :, columns]], axis=0)
    return total + jnp.dot(x, w, preferred_element_type=jnp.float32)


def near_kernel(w_mine, w_other, *refs):
    *pieces, out = refs
    width = out.shape[1] // 2
    for start in range(0, out.shape[0], BLOCK):
        rows = slice(start, start + BLOCK)
        for side in range(2):
            columns = slice(side * width, (side + 1) * width)
            total = jnp.zeros((BLOCK, width), jnp.float32)
            for x, s in zip(pieces, (0, 1, 3, 4, 5, 7)):
                total = add_product(total, x[rows], s, w_mine, w_other, columns)
            out[rows, columns] = total


def hidden_kernel(w_mine, w_other, low0, high0, low1, high1, sums, out):
    copies, zs, cores = 4, 8, 2
    n, half_width = out.shape[1], out.shape[2]
    width, cut = cores * half_width, low0.shape[0]
    for start in range(0, sums.shape[0], BLOCK):
        rows = slice(start, start + BLOCK)
        if start < cut:
            x0, x1 = low0[rows], low1[rows]
        else:
            x0, x1 = high0[start - cut : start - cut + BLOCK], high1[start - cut : start - cut + BLOCK]
        for c in range(cores):
            both = []
            for first in (c * half_width, width + c * half_width):
                columns = slice(first, first + half_width)
                total = add_product(sums[rows, columns], x0, 2, w_mine, w_other, columns)
                both.append(add_product(total, x1, 6, w_mine, w_other, columns))
            gate, up = both
            active = (gate / (1.0 + jnp.exp(-gate)) * up).astype(jnp.bfloat16)
            for j in range(BLOCK // n):
                z, row = divmod(start // n + j, copies)
                out[(c * zs + z) * copies + row] = active[j * n : (j + 1) * n]


def on_core(kernel, out_shape, *inputs):
    vmem = pl.BlockSpec(memory_space=pltpu.VMEM)
    return pl.pallas_call(
        kernel,
        out_shape=out_shape,
        in_specs=[vmem] * len(inputs),
        out_specs=vmem,
        cost_estimate=pl.CostEstimate(
            flops=768 * 3072 * 1024, bytes_accessed=6 * 2**20, transcendentals=768 * 512
        ),
        compiler_params=pltpu.CompilerParams(vmem_limit_bytes=12 * 2**20),
    )(*inputs)


def gather_x(block, later):
    half = block.shape[0] // 2
    low = lax.ppermute(block, "x", shift("x", 1))
    high = lax.ppermute(block, "x", shift("x", -1))
    low_part, high_part = low[:half], high[half:]
    low_part, high_part, later = lax.optimization_barrier((low_part, high_part, later))
    far_a = lax.ppermute(low_part, "x", shift("x", 1))
    far_b = lax.ppermute(high_part, "x", shift("x", -1))
    return (block, low, high, far_a, far_b), later


def local(tokens, expert_ids, joined_weight):
    zs, copies = lax.axis_size("z"), lax.axis_size("yh")
    yls, xs, cores = lax.axis_size("yl"), lax.axis_size("x"), lax.axis_size("c")
    chips = yls * xs
    part = CAP // cores
    core, here, side = lax.axis_index("c"), lax.axis_index("x"), lax.axis_index("yl")
    rows = joined_weight.shape[1]
    chip_width = joined_weight.shape[3] // chips
    half_width = chip_width // cores

    tok_count = tokens.shape[0]
    flat_ids = expert_ids.reshape(-1)
    chosen = (flat_ids[:, None] == jnp.arange(E, dtype=jnp.int32)[None, :]).astype(jnp.int32)
    earlier = jnp.cumsum(chosen, axis=0) - chosen
    position = jnp.sum(earlier * chosen, axis=1)
    slot_index = flat_ids * part + position + (position >= part) * (E * part - part)
    slots = jnp.arange(E * CAP, dtype=jnp.int32)
    pick_table = (slot_index[:, None] == slots[None, :]).astype(jnp.bfloat16)
    token_table = pick_table.reshape(tok_count, TOP, E * CAP).sum(axis=1)
    placed = lax.dot_general(
        token_table, tokens, (((0,), (0,)), ((), ())), preferred_element_type=jnp.float32
    ).astype(jnp.bfloat16)

    sent = placed.reshape(cores, zs, 1, part, rows)
    sent = jnp.broadcast_to(sent, (cores, zs, copies, part, rows)).reshape(-1, part, rows)
    got = lax.all_to_all(sent, ("c", "z", "yh"), 0, 0, tiled=True)
    got = got.reshape(cores, zs * copies, part, rows)

    turn = jnp.arange(chips, dtype=jnp.int32)
    chip = lax.rem(side + turn // xs, yls) * xs + lax.rem(here + turn % xs, xs)
    pieces = split_columns(joined_weight, chip)
    moved = [pieces[0]]
    for s in range(1, chips):
        moved.append(lax.ppermute(pieces[s], CHIPS, chip_shift(s // xs, s % xs)))
    mine = jnp.where(core == 0, got[0], got[1])
    theirs = jnp.where(core == 0, got[1], got[0])
    own = jnp.concatenate([mine, theirs], axis=-1).reshape(zs * copies * part, cores * rows)
    opposite = lax.ppermute(own, "yl", SWAP)
    near, moved = gather_x(own, moved)
    w_mine = jnp.concatenate([m.reshape(rows, 2 * chip_width) for m in moved], axis=0)
    w_other = lax.ppermute(w_mine, "c", SWAP)
    shape = (chips, rows, 2 * chip_width)
    w_mine, w_other = w_mine.reshape(shape), w_other.reshape(shape)

    far, _ = gather_x(opposite, ())
    sums = jax.ShapeDtypeStruct((own.shape[0], 2 * chip_width), jnp.float32)
    half_sums = on_core(near_kernel, sums, w_mine, w_other, *near[:3], *far[:3])
    active = jax.ShapeDtypeStruct((zs * copies * cores, part, half_width), jnp.bfloat16)
    outgoing = on_core(hidden_kernel, active, w_mine, w_other, *near[3:], *far[3:], half_sums)

    pick_table, outgoing = lax.optimization_barrier((pick_table, outgoing))
    returned = lax.all_to_all(outgoing, ("c", "z", "yh"), 0, 0, tiled=True)
    grouped = returned.reshape(cores * E, copies, part, half_width).transpose(0, 2, 1, 3)
    grouped = grouped.reshape(E * CAP, copies * half_width)
    hidden = jnp.dot(pick_table, grouped, preferred_element_type=jnp.float32).astype(jnp.bfloat16)
    return hidden.reshape(tok_count, TOP, copies, half_width)


def solution(mesh):
    fine = Mesh(mesh.devices.reshape(8, 4, 2, 4, 2), ("z", "yh", "yl", "x", "c"))

    return jax.shard_map(
        local,
        mesh=fine,
        in_specs=(P(EXPERT, TENSOR), P(EXPERT, None), P(EXPERT, TENSOR, None, None)),
        out_specs=P(EXPERT, None, None, TENSOR),
        check_vma=False,
    )
```
